256 devices in a mesh: dp: 64 (over z, x, core), tensor: 4 (over y).
Axes of the slice: x: 4, y: 4, z: 8, core: 2. Of those that a mesh axis runs over, the one named last changes fastest.
Arguments:
- inputs: bfloat16 [2, 16384, 1280], P(None, 'dp'), may hold values from -16 to 16
- cotangent: bfloat16 [2, 16384, 1280], P(None, 'dp'), may hold values from -0.4375 to 0.4375
- w_in: bfloat16 [1280, 5120], P('dp', 'tensor'), may hold values from -0.15625 to 0.15625
- w_out: bfloat16 [1280, 5120], P('dp', 'tensor'), may hold values from -0.078125 to 0.078125
- grad_in: float32 [1280, 5120], P('dp', 'tensor'), may hold values from -24 to 24
- grad_out: float32 [1280, 5120], P('dp', 'tensor'), may hold values from -24 to 24
Outputs:
- branch_output: bfloat16 [2, 16384, 1280], P(None, 'dp', 'tensor')
- ascent_in: float32 [1280, 5120], P('dp', 'tensor')
- ascent_out: float32 [1280, 5120], P('dp', 'tensor')
- new_grad_in: float32 [1280, 5120], P('dp', 'tensor')
- new_grad_out: float32 [1280, 5120], P('dp', 'tensor')
The draws below stay inside these ranges and needn't reach their ends.
All inputs are finite; a program needn't handle non-finite values.
Results may differ from the reference program's by a relative error of at most 0.0064.
Values may be sent and summed in bfloat16 or wider, within the bound.
No kernel may reach another device: no remote copies, remote signals or barrier semaphores. Data moves between devices by JAX's collectives and lax.ppermute only.
A program may use at most 128 MiB of HBM per device.

```python
import math
import jax
import jax.numpy as jnp
from jax import lax

D = 1280
FF = 5120
MB = 2
TOKENS = 16384


def grad_table(key, rows, cols):
    key_rows, key_vals, key_common = jax.random.split(key, 3)
    scales = jnp.exp(jax.random.uniform(key_rows, (rows, 1), jnp.float32, math.log(0.25), math.log(4.0)))
    values = jnp.clip(jax.random.normal(key_vals, (rows, cols), jnp.float32), -6.0, 6.0)
    return jnp.clip(values * scales, -24.0, 24.0)


def draw_grad_in(key, part):
    return grad_table(jax.random.fold_in(key, 11), D, FF)


def draw_grad_out(key, part):
    return grad_table(jax.random.fold_in(key, 23), D, FF)


def with_spikes(values, rng, source, target, parts, factor):
    def block_of(position):
        return (jnp.arange(values.shape[position]) // (values.shape[position] // parts)).reshape((-1,) + (1,) * (values.ndim - 1 - position))

    one_side = jax.random.permutation(rng, parts)[block_of(target)]
    far = (block_of(target) + parts // 2) % parts
    return jnp.where((block_of(source) == one_side) | (block_of(source) == far), factor * values, values)


def shard_levels(key, dims, cuts, smallest, high):
    level = 1.0
    for dim, shards_of in cuts:
        draws = jax.random.uniform(jax.random.fold_in(jax.random.fold_in(key, 6), dim), (shards_of,), jnp.float32, smallest / len(cuts), high / len(cuts))
        level = level * jnp.repeat(jnp.exp(draws), dims[dim] // shards_of).reshape((-1,) + (1,) * (len(dims) - 1 - dim))
    return level


def noise(stream_key, extent, width, reach, cuts=(), held_as=jnp.bfloat16):
    values = width * jax.random.normal(stream_key, extent, jnp.float32)
    if cuts:
        values = values * shard_levels(stream_key, extent, cuts, -0.22, 0.18)
    return jnp.clip(values, -reach, reach).astype(held_as)


def bell_draw_with(stream_key, dims, spread, bound, pieces, heavy, kind=jnp.bfloat16):
    drawn = spread * jax.random.normal(stream_key, dims, jnp.float32)
    if pieces:
        drawn = drawn * shard_levels(stream_key, dims, pieces, -0.22, 0.18)
    return jnp.clip(with_spikes(drawn, jax.random.fold_in(stream_key, 3), *heavy), -bound, bound).astype(kind)


def setup_inputs(seed: int = 0) -> dict:
    splits = jax.random.split(jax.random.key(seed), 7)
    inputs = bell_draw_with(splits[0], (MB, TOKENS, D), 1.0, 16.0, ((1, 64),), (1, 2, 64, 4.0))
    cotangent = bell_draw_with(splits[1], (MB, TOKENS, D), (2.0 / (2 * TOKENS) ** 0.5), 0.4375, ((1, 64),), (1, 2, 64, 4.0))
    w_in = noise(splits[2], (D, FF), D ** -0.5, 0.15625, ((0, 64), (1, 4)))
    w_out = noise(splits[3], (D, FF), FF ** -0.5, 0.078125, ((0, 64), (1, 4)))
    grad_in = draw_grad_in(jax.random.fold_in(splits[6], 71), 0)
    grad_out = draw_grad_out(jax.random.fold_in(splits[6], 71), 0)
    return {"inputs": inputs, "cotangent": cotangent, "w_in": w_in, "w_out": w_out, "grad_in": grad_in, "grad_out": grad_out}


RHO = 0.1
ETA = 0.01

def gelu_parts(pre):
    cdf = 0.5 * (1.0 + lax.erf(pre * 0.7071067811865476))
    dens = jnp.exp(-0.5 * pre * pre) * 0.3989422804014327
    return (pre * cdf, cdf + pre * dens)

def reference(inputs, cotangent, w_in, w_out, grad_in, grad_out):
    scale_in = jnp.abs(w_in.astype(jnp.float32)) + ETA
    scale_out = jnp.abs(w_out.astype(jnp.float32)) + ETA
    scaled_in = scale_in * grad_in
    scaled_out = scale_out * grad_out
    total = jnp.sum(scaled_in * scaled_in) + jnp.sum(scaled_out * scaled_out)
    factor = math.sqrt(2.0 * D * FF) / jnp.sqrt(total + 1.0)
    ascent_in = factor * scaled_in
    ascent_out = factor * scaled_out
    moved_in = (w_in.astype(jnp.float32) + RHO * scale_in * ascent_in).astype(jnp.bfloat16)
    moved_out = (w_out.astype(jnp.float32) + RHO * scale_out * ascent_out).astype(jnp.bfloat16)
    outputs = []
    new_in = jnp.zeros((D, FF), jnp.float32)
    new_out = jnp.zeros((D, FF), jnp.float32)
    for index in range(MB):
        rows = inputs[index]
        grads_y = cotangent[index]
        pre = jnp.dot(rows, moved_in, preferred_element_type=jnp.float32)
        act, slope = gelu_parts(pre)
        act = act.astype(jnp.bfloat16)
        result = jnp.dot(act, moved_out.T, preferred_element_type=jnp.float32)
        outputs.append(result.astype(jnp.bfloat16))
        back = jnp.dot(grads_y, moved_out, preferred_element_type=jnp.float32)
        delta = (back * slope).astype(jnp.bfloat16)
        new_in = new_in + jnp.dot(rows.T, delta, preferred_element_type=jnp.float32)
        new_out = new_out + jnp.dot(grads_y.T, act, preferred_element_type=jnp.float32)
    return (jnp.stack(outputs), ascent_in, ascent_out, new_in, new_out)
```

```python
import math

import jax
import jax.numpy as jnp
from jax import lax
from jax.sharding import Mesh, PartitionSpec as P

D = 1280
FF = 5120

RHO = 0.1
ETA = 0.01


Z, X, C, Y = 8, 4, 2, 4
CHIP = D // (Z * X)
COL = CHIP * X
HALF = FF // Y // C
SIZES = {"z": Z, "x": X, "c": C, "y": Y}
F32, BF16 = jnp.float32, jnp.bfloat16


def shift(a, axis, by):
    n = SIZES[axis]
    return lax.ppermute(a, axis, [(i, (i + by) % n) for i in range(n)])


def sum_over(part, axes, count):
    copies = jnp.broadcast_to(part.reshape(1, 1), (count, 1, 1))
    return jnp.sum(lax.all_to_all(copies, axes, 0, 0, tiled=True))


def dot(a, b, da, db):
    return lax.dot_general(a, b, (((da,), (db,)), ((), ())), preferred_element_type=F32)


def gelu_parts(pre):
    cdf = 0.5 * (1.0 + lax.erf(pre * 0.7071067811865476))
    dens = jnp.exp(-0.5 * pre * pre) * 0.3989422804014327
    return (pre * cdf, cdf + pre * dens)


def local(inputs, cotangent, w_in, w_out, grad_in, grad_out):
    z, x, c = (lax.axis_index(a) for a in ("z", "x", "c"))
    first = c == 0

    scale_in = jnp.abs(w_in.astype(F32)) + ETA
    scale_out = jnp.abs(w_out.astype(F32)) + ETA
    scaled_in = scale_in * grad_in
    scaled_out = scale_out * grad_out
    part = jnp.sum(scaled_in * scaled_in) + jnp.sum(scaled_out * scaled_out)
    part = part + shift(part.reshape(1, 1), "c", 1)[0, 0]
    part = sum_over(part, ("x", "y"), X * Y)
    total = sum_over(part, "z", Z)
    factor = math.sqrt(2.0 * D * FF) / jnp.sqrt(total + 1.0)
    ascent_in = factor * scaled_in
    ascent_out = factor * scaled_out

    raw = jnp.stack([w_in, w_out, grad_in.astype(BF16), grad_out.astype(BF16)])
    low, high = raw[:, :, :HALF], raw[:, :, HALF:]
    mine, other = jnp.where(first, low, high), jnp.where(first, high, low)
    came = shift(other, "c", 1)
    chip = jnp.where(first, jnp.concatenate([mine, came], 1), jnp.concatenate([came, mine], 1))
    row = jnp.concatenate([chip, shift(chip, "x", -1), shift(chip, "x", 2), shift(chip, "x", 1)], 1)

    def moved(w, g):
        w, g = w.astype(F32), g.astype(F32)
        scale = jnp.abs(w) + ETA
        return (w + RHO * scale * (factor * (scale * g))).astype(BF16)

    start_in, start_out = moved(row[0], row[2]), moved(row[1], row[3])

    r = lax.broadcasted_iota(jnp.int32, (D, 1), 0)
    at = ((r // COL + z) % Z) * COL + ((r % COL // CHIP + x) % X) * CHIP + r % CHIP
    turn = (at == lax.broadcasted_iota(jnp.int32, (1, D), 1)).astype(BF16)

    def features(a):
        own = dot(turn, a.reshape(-1, D), 1, 1).astype(BF16)
        return jnp.concatenate([own, shift(own, "c", 1)], 1)

    xt, dyt = features(inputs), features(cotangent)

    def gathered(block, up):
        blocks = [None] * Z
        blocks[0] = block
        a = b = block
        for k in range(1, Z // 2 + 1):
            if k < Z // 2 or up:
                a = shift(a, "z", -1)
                blocks[k] = a
            if k < Z // 2 or not up:
                b = shift(b, "z", 1)
                blocks[Z - k] = b
        return jnp.concatenate(blocks, 0)

    full_in = gathered(start_in, True)
    full_out = gathered(start_out, False)

    pre = dot(full_in, xt, 0, 0)
    act, slope = gelu_parts(pre)
    act = act.astype(BF16)
    back = dot(full_out, dyt, 0, 0)
    delta = (back * slope).astype(BF16)

    def reduced(left, right, up):
        def block(k):
            return dot(left[k * COL : (k + 1) * COL], right, 1, 1)

        far_up, far_down = (4, 5) if up else (3, 4)
        a, b = block(far_up), block(far_down)
        for k in range(far_up - 1, 0, -1):
            a = block(k) + shift(a.astype(BF16), "z", 1).astype(F32)
        for k in range(far_down + 1, Z):
            b = block(k) + shift(b.astype(BF16), "z", -1).astype(F32)
        ends = shift(a.astype(BF16), "z", 1), shift(b.astype(BF16), "z", -1)
        return block(0) + ends[0].astype(F32) + ends[1].astype(F32)

    sums = jnp.stack([reduced(xt, delta, True), reduced(dyt, act, False)])
    chip_sum = sums[:, :CHIP]
    for j in range(1, X):
        piece = sums[:, j * CHIP : (j + 1) * CHIP].astype(BF16)
        chip_sum = chip_sum + shift(piece, "x", j if j < 3 else -1).astype(F32)
    top, bottom = chip_sum[:, : CHIP // 2], chip_sum[:, CHIP // 2 :]
    keep, give = jnp.where(first, top, bottom), jnp.where(first, bottom, top)
    got = shift(give, "c", 1)
    new = jnp.where(first, jnp.concatenate([keep, got], 2), jnp.concatenate([got, keep], 2))

    plain_out = dot(turn, full_out, 0, 0).astype(BF16)
    y = dot(plain_out, act, 1, 0)
    tokens = y.shape[1] // C
    own = y[:, :tokens] + shift(y[:, tokens:].astype(BF16), "c", 1).astype(F32)
    parts = lax.all_to_all(own.astype(BF16).reshape(Y, D // Y, tokens), "y", 0, 0, tiled=True)
    branch = jnp.sum(parts.astype(F32), 0).astype(BF16).T.reshape(*inputs.shape[:2], D // Y)
    return (branch, ascent_in, ascent_out, new[0], new[1])


def solution(mesh):
    grid = Mesh(mesh.devices.reshape(Z, X, C, Y), ("z", "x", "c", "y"))
    dp = ("z", "x", "c")
    return jax.shard_map(
        local,
        mesh=grid,
        in_specs=(P(None, dp, None), P(None, dp, None)) + (P(dp, "y"),) * 4,
        out_specs=(P(None, dp, "y"),) + (P(dp, "y"),) * 4,
        check_vma=False,
    )
```

```python
import math

import jax
import jax.numpy as jnp
from jax import lax
from jax.experimental import pallas as pl
from jax.experimental.pallas import tpu as pltpu
from jax.sharding import Mesh, PartitionSpec as P


D = 1280
FF = 5120

RHO = 0.1
ETA = 0.01


Z, X, C, Y = 8, 4, 2, 4
CHIP = D // (Z * X)
COL = CHIP * X
HALF = FF // Y // C
TILE = 256
SIZES = {"z": Z, "x": X, "c": C, "y": Y}
F32, BF16 = jnp.float32, jnp.bfloat16


def shift(a, axis, by):
    n = SIZES[axis]
    return lax.ppermute(a, axis, [(i, (i + by) % n) for i in range(n)])


def exchanged(parts, axis):
    return lax.all_to_all(parts, axis, 0, 0, tiled=True)


def sum_over(part, axes, count):
    return jnp.sum(exchanged(jnp.broadcast_to(part.reshape(1, 1), (count, 1, 1)), axes))


def turned(blocks, axis):
    n = SIZES[axis]
    start = lax.rem(n - lax.axis_index(axis), n)
    return lax.dynamic_slice_in_dim(jnp.concatenate([blocks, blocks], 0), start, n, 0)


def gelu_parts(pre):
    cdf = 0.5 * (1.0 + lax.erf(pre * 0.7071067811865476))
    dens = jnp.exp(-0.5 * pre * pre) * 0.3989422804014327
    return (pre * cdf, cdf + pre * dens)


def dot(a, b, da, db):
    return lax.dot_general(a, b, (((da,), (db,)), ((), ())), preferred_element_type=F32)


def act_kernel(x_ref, w_ref, act_ref, slope_ref, pre_ref):
    pre_ref[...] = dot(x_ref[...], w_ref[...], 1, 0)

    def some(i, carry):
        rows = pl.ds(pl.multiple_of(i * 16, 16), 16)
        act, slope = gelu_parts(pre_ref[rows])
        act_ref[rows] = act.astype(BF16)
        slope_ref[rows] = slope
        return carry

    lax.fori_loop(0, TILE // 16, some, 0)


def delta_kernel(dy_ref, w_ref, slope_ref, delta_ref):
    delta_ref[...] = (dot(dy_ref[...], w_ref[...], 1, 0) * slope_ref[...]).astype(BF16)


def grad_kernel(x_ref, d_ref, g_ref):
    g_ref[...] = dot(x_ref[...], d_ref[...], 0, 0)


def out_kernel(w_ref, act_ref, y_ref):
    y_ref[...] = dot(w_ref[...], act_ref[...], 1, 1).astype(BF16)


def call(kernel, steps, operands, blocks, outs, out_blocks, scratch=()):
    spec = lambda shape, cut: pl.BlockSpec(
        tuple(TILE if i == cut else s for i, s in enumerate(shape)),
        lambda i: tuple(i if j == cut else 0 for j in range(len(shape))),
    )
    many = len(outs) > 1
    shapes = [jax.ShapeDtypeStruct(*o) for o in outs]
    out_specs = [spec(o[0], cut) for o, cut in zip(outs, out_blocks)]
    return pl.pallas_call(
        kernel,
        grid=(steps,),
        in_specs=[spec(o.shape, cut) for o, cut in zip(operands, blocks)],
        out_specs=out_specs if many else out_specs[0],
        out_shape=shapes if many else shapes[0],
        scratch_shapes=list(scratch),
        cost_estimate=pl.CostEstimate(flops=2 * 1024 * D * HALF, bytes_accessed=8 << 20, transcendentals=0),
    )(*operands)


def local(inputs, cotangent, w_in, w_out, grad_in, grad_out):
    z, c = lax.axis_index("z"), lax.axis_index("c")
    first = c == 0

    raw = jnp.stack([w_in, grad_in.astype(BF16), w_out, grad_out.astype(BF16)])
    low, high = raw[:, :, :HALF], raw[:, :, HALF:]
    mine, other = jnp.where(first, low, high), jnp.where(first, high, low)
    came = shift(other, "c", 1)
    chip = jnp.where(first, jnp.concatenate([mine, came], 1), jnp.concatenate([came, mine], 1))
    chip, grad_in, grad_out = lax.optimization_barrier((chip, grad_in, grad_out))
    row = turned(jnp.stack([chip] + [shift(chip, "x", -j if j < 3 else 1) for j in range(1, X)]), "x")
    own = jnp.stack([inputs.reshape(-1, D), cotangent.reshape(-1, D)])
    tokens = own.shape[1]
    came = shift(own, "c", 1)
    x = jnp.concatenate([own[0], came[0]], 0)
    dy = jnp.concatenate([own[1], came[1]], 0)
    count = x.shape[0]

    scaled_in = (jnp.abs(w_in.astype(F32)) + ETA) * grad_in
    scaled_out = (jnp.abs(w_out.astype(F32)) + ETA) * grad_out
    part = jnp.sum(scaled_in * scaled_in) + jnp.sum(scaled_out * scaled_out)
    part = sum_over(part, ("x", "c", "y"), X * C * Y)
    total = sum_over(part, "z", Z)
    factor = math.sqrt(2.0 * D * FF) / jnp.sqrt(total + 1.0)
    ascent_in = factor * scaled_in
    ascent_out = factor * scaled_out

    def moved(w, g):
        w, g = w.astype(F32), g.astype(F32)
        scale = jnp.abs(w) + ETA
        new = (w + RHO * scale * (factor * (scale * g))).astype(BF16)
        return new.reshape(COL, HALF)

    start_in, start_out = moved(row[:, 0], row[:, 1]), moved(row[:, 2], row[:, 3])

    def place(k):
        return lax.rem(z + k, Z)

    def gathered(block, up):
        full = jnp.zeros((Z, COL, HALF), BF16)
        put = lambda full, block, k: lax.dynamic_update_index_in_dim(full, block, place(k), 0)
        full = put(full, block, 0)
        a = b = block
        for k in range(1, Z // 2 + 1):
            if k < Z // 2 or up:
                a = shift(a, "z", -1)
                full = put(full, a, k)
            if k < Z // 2 or not up:
                b = shift(b, "z", 1)
                full = put(full, b, Z - k)
        return full.reshape(D, HALF)

    full_in = gathered(start_in, True)
    full_out = gathered(start_out, False)

    hidden = (count, HALF)
    act, slope = call(
        act_kernel, count // TILE, (x, full_in), (0, None),
        ((hidden, BF16), (hidden, F32)), (0, 0), [pltpu.VMEM((TILE, HALF), F32)],
    )
    whole_out = call(grad_kernel, D // TILE, (dy, act), (1, None), (((D, HALF), F32),), (0,))
    delta = call(delta_kernel, count // TILE, (dy, full_out, slope), (0, None, 0), ((hidden, BF16),), (0,))
    whole_in = call(grad_kernel, D // TILE, (x, delta), (1, None), (((D, HALF), F32),), (0,))

    def reduced(whole, up):
        blocks = whole.reshape(Z, COL, HALF)

        def block(k):
            return lax.dynamic_index_in_dim(blocks, place(k), 0, keepdims=False)

        far_up, far_down = (4, 5) if up else (3, 4)
        a, b = block(far_up), block(far_down)
        for k in range(far_up - 1, -1, -1):
            a = block(k) + shift(a.astype(BF16), "z", 1).astype(F32)
        for k in range(far_down + 1, Z):
            b = block(k) + shift(b.astype(BF16), "z", -1).astype(F32)
        return a + shift(b.astype(BF16), "z", -1).astype(F32)

    sums = jnp.stack([reduced(whole_in, True), reduced(whole_out, False)])

    y = call(out_kernel, D // TILE, (full_out, act), (0, None), (((D, count), BF16),), (0,))
    mixed = y[:, :tokens].astype(F32) + shift(y[:, tokens:], "c", 1).astype(F32)
    parts = exchanged(mixed.astype(BF16).reshape(Y, D // Y, tokens), "y")

    pieces = sums.astype(BF16).reshape(2, X, CHIP, HALF).swapaxes(0, 1)
    pieces, parts = lax.optimization_barrier((pieces, parts))
    chip_sum = jnp.sum(exchanged(pieces, "x").astype(F32), 0)
    top, bottom = chip_sum[:, : CHIP // 2], chip_sum[:, CHIP // 2 :]
    keep, give = jnp.where(first, top, bottom), jnp.where(first, bottom, top)
    got = shift(give, "c", 1)
    new = jnp.where(first, jnp.concatenate([keep, got], 2), jnp.concatenate([got, keep], 2))

    branch = jnp.sum(parts.astype(F32), 0).astype(BF16).T.reshape(*inputs.shape[:2], D // Y)
    return (branch, ascent_in, ascent_out, new[0], new[1])


def solution(mesh):
    grid = Mesh(mesh.devices.reshape(Z, X, C, Y), ("z", "x", "c", "y"))
    dp = ("z", "x", "c")

    return jax.shard_map(
        local,
        mesh=grid,
        in_specs=(P(None, dp, None), P(None, dp, None)) + (P(dp, "y"),) * 4,
        out_specs=(P(None, dp, "y"),) + (P(dp, "y"),) * 4,
        check_vma=False,
    )
```

```python
import functools
import math

import jax
import jax.numpy as jnp
from jax import lax
from jax.experimental import pallas as pl
from jax.experimental.pallas import tpu as pltpu
from jax.sharding import Mesh, PartitionSpec as P


D = 1280
FF = 5120

RHO = 0.1
ETA = 0.01


Z, X, C, Y = 8, 4, 2, 4
CHIP = D // (Z * X)
COL = CHIP * X
HALF = FF // Y // C
TILE = 256
SIZES = {"z": Z, "x": X, "c": C, "y": Y}
F32, BF16 = jnp.float32, jnp.bfloat16


def shift(a, axis, by):
    n = SIZES[axis]
    return lax.ppermute(a, axis, [(i, (i + by) % n) for i in range(n)])


def exchanged(parts, axis):
    return lax.all_to_all(parts, axis, 0, 0, tiled=True)


def sum_over(part, axes, count):
    return jnp.sum(exchanged(jnp.broadcast_to(part.reshape(1, 1), (count, 1, 1)), axes))


def gelu_parts(pre):
    cdf = 0.5 * (1.0 + lax.erf(pre * 0.7071067811865476))
    dens = jnp.exp(-0.5 * pre * pre) * 0.3989422804014327
    return (pre * cdf, cdf + pre * dens)


def dot(a, b, da, db):
    return lax.dot_general(a, b, (((da,), (db,)), ((), ())), preferred_element_type=F32)


def by_owner(own_ref, came_ref, work):
    steps = pl.num_programs(0) // 2

    @pl.when(pl.program_id(0) < steps)
    def _():
        work(own_ref[...])

    @pl.when(pl.program_id(0) >= steps)
    def _():
        work(came_ref[...])


def act_kernel(own_ref, came_ref, w_ref, act_ref, slope_ref, pre_ref):
    def product(x):
        pre_ref[...] = dot(x, w_ref[...], 1, 0)

    by_owner(own_ref, came_ref, product)

    def some(i, carry):
        rows = pl.ds(pl.multiple_of(i * 16, 16), 16)
        act, slope = gelu_parts(pre_ref[rows])
        act_ref[rows] = act.astype(BF16)
        slope_ref[rows] = slope
        return carry

    lax.fori_loop(0, TILE // 16, some, 0)


def delta_kernel(own_ref, came_ref, w_ref, slope_ref, delta_ref):
    def product(dy):
        delta_ref[...] = (dot(dy, w_ref[...], 1, 0) * slope_ref[...]).astype(BF16)

    by_owner(own_ref, came_ref, product)


def grad_kernel(own_ref, came_ref, d_ref, g_ref):
    half = own_ref.shape[0]
    g_ref[...] = dot(own_ref[...], d_ref[:half], 0, 0) + dot(came_ref[...], d_ref[half:], 0, 0)


def out_kernel(w_ref, act_ref, own_ref, other_ref):
    half = own_ref.shape[1]
    own_ref[...] = dot(w_ref[...], act_ref[:half], 1, 1).astype(BF16)
    other_ref[...] = dot(w_ref[...], act_ref[half:], 1, 1).astype(BF16)


def add_kernel(k, whole_ref, *refs):
    at = lax.rem(lax.axis_index("z") + k, Z)

    def some(i, carry):
        rows = pl.ds(pl.multiple_of(i * 32, 32), 32)
        total = whole_ref[at, rows]
        for came in refs[:-1]:
            total = total + came[rows].astype(F32)
        refs[-1][rows] = total.astype(BF16)
        return carry

    lax.fori_loop(0, COL // 32, some, 0)


def added(whole, k, *came):
    return pl.pallas_call(
        functools.partial(add_kernel, k),
        out_shape=jax.ShapeDtypeStruct((COL, HALF), BF16),
        in_specs=[pl.BlockSpec(memory_space=pltpu.VMEM)] * (1 + len(came)),
        out_specs=pl.BlockSpec(memory_space=pltpu.VMEM),
        compiler_params=pltpu.CompilerParams(vmem_limit_bytes=6 << 20),
        cost_estimate=pl.CostEstimate(flops=1 << 19, bytes_accessed=1 << 20, transcendentals=0),
    )(whole, *came)


def call(kernel, steps, operands, outs, scratch=()):
    def spec(shape, cut, at):
        block = tuple(TILE if i == cut else n for i, n in enumerate(shape))
        return pl.BlockSpec(block, lambda i: tuple(at(i) if j == cut else 0 for j in range(len(shape))))

    shapes = [jax.ShapeDtypeStruct(*o[0]) for o in outs]
    return pl.pallas_call(
        kernel,
        grid=(steps,),
        in_specs=[spec(o.shape, cut, at) for o, cut, at in operands],
        out_specs=[spec(o[0], cut, at) for o, cut, at in outs],
        out_shape=shapes,
        scratch_shapes=list(scratch),
        compiler_params=pltpu.CompilerParams(vmem_limit_bytes=14 << 20),
        cost_estimate=pl.CostEstimate(flops=2 * 1024 * D * HALF, bytes_accessed=8 << 20, transcendentals=0),
    )(*[o[0] for o in operands])


def same(i):
    return i


def local(inputs, cotangent, w_in, w_out, grad_in, grad_out):
    z, c = lax.axis_index("z"), lax.axis_index("c")
    first = c == 0

    scaled_in = (jnp.abs(w_in.astype(F32)) + ETA) * grad_in
    scaled_out = (jnp.abs(w_out.astype(F32)) + ETA) * grad_out
    part = jnp.sum(scaled_in * scaled_in) + jnp.sum(scaled_out * scaled_out)
    part, w_in, w_out, grad_in, grad_out = lax.optimization_barrier((part, w_in, w_out, grad_in, grad_out))
    part = sum_over(part, ("x", "c", "y"), X * C * Y)

    raw = jnp.stack([w_in, grad_in.astype(BF16), w_out, grad_out.astype(BF16)])
    low, high = raw[:, :, :HALF], raw[:, :, HALF:]
    mine, other = jnp.where(first, low, high), jnp.where(first, high, low)
    came = shift(other, "c", 1)
    chip = jnp.where(first, jnp.concatenate([mine, came], 1), jnp.concatenate([came, mine], 1))
    chip, grad_in, grad_out = lax.optimization_barrier((chip, grad_in, grad_out))
    near = [chip] + [shift(chip, "x", -j if j < 3 else 1) for j in range(1, X)]
    x, dy = inputs.reshape(-1, D), cotangent.reshape(-1, D)
    x_came, dy_came = shift(x, "c", 1), shift(dy, "c", 1)
    tokens = x.shape[0]
    count = C * tokens

    total = sum_over(part, "z", Z)
    factor = math.sqrt(2.0 * D * FF) / jnp.sqrt(total + 1.0)
    ascent_in = factor * ((jnp.abs(w_in.astype(F32)) + ETA) * grad_in)
    ascent_out = factor * ((jnp.abs(w_out.astype(F32)) + ETA) * grad_out)

    def moved(w, g):
        w, g = w.astype(F32), g.astype(F32)
        scale = jnp.abs(w) + ETA
        return (w + RHO * scale * (factor * (scale * g))).astype(BF16)

    def row(which):
        at = lax.axis_index("x")
        by_x = [lax.select_n(at, *[near[(a - b) % X] for b in range(X)]) for a in range(X)]
        return jnp.concatenate([moved(r[which], r[which + 1]) for r in by_x], 0)

    start_in, start_out = row(0), row(2)

    def place(k):
        return lax.rem(z + k, Z)

    def gathered(block, up):
        full = jnp.zeros((Z, COL, HALF), BF16)
        put = lambda full, block, k: lax.dynamic_update_index_in_dim(full, block, place(k), 0)
        full = put(full, block, 0)
        a = b = block
        for k in range(1, Z // 2 + 1):
            if k < Z // 2 or up:
                a = shift(a, "z", -1)
                full = put(full, a, k)
            if k < Z // 2 or not up:
                b = shift(b, "z", 1)
                full = put(full, b, Z - k)
        return full.reshape(D, HALF)

    full_in = gathered(start_in, True)
    full_out = gathered(start_out, False)

    hidden, square = (count, HALF), (D, HALF)
    half = tokens // TILE
    pair = lambda own, came: ((own, 0, lambda i: jnp.minimum(i, half - 1)), (came, 0, lambda i: jnp.maximum(i - half, 0)))
    act, slope = call(
        act_kernel, count // TILE, (*pair(x, x_came), (full_in, None, same)),
        (((hidden, BF16), 0, same), ((hidden, F32), 0, same)), [pltpu.VMEM((TILE, HALF), F32)],
    )
    (whole_out,) = call(
        grad_kernel, D // TILE, ((dy, 1, same), (dy_came, 1, same), (act, None, same)), (((square, F32), 0, same),)
    )
    (delta,) = call(
        delta_kernel, count // TILE, (*pair(dy, dy_came), (full_out, None, same), (slope, 0, same)),
        (((hidden, BF16), 0, same),),
    )
    (whole_in,) = call(
        grad_kernel, D // TILE, ((x, 1, same), (x_came, 1, same), (delta, None, same)), (((square, F32), 0, same),)
    )

    def reduced(whole, up):
        whole = whole.reshape(Z, COL, HALF)
        far_up, far_down = (4, 5) if up else (3, 4)
        a, b = added(whole, far_up), added(whole, far_down)
        for k in range(far_up - 1, 0, -1):
            a = added(whole, k, shift(a, "z", 1))
        for k in range(far_down + 1, Z):
            b = added(whole, k, shift(b, "z", -1))
        return added(whole, 0, shift(a, "z", 1), shift(b, "z", -1))

    sums = jnp.stack([reduced(whole_in, True), reduced(whole_out, False)])

    out = (((D, tokens), BF16), 0, same)
    own, other = call(out_kernel, D // TILE, ((full_out, 0, same), (act, None, same)), (out, out))
    mixed = own.astype(F32) + shift(other, "c", 1).astype(F32)
    parts = exchanged(mixed.astype(BF16).reshape(Y, D // Y, tokens), "y")

    pieces = sums.reshape(2, X, CHIP, HALF).swapaxes(0, 1)
    pieces, parts = lax.optimization_barrier((pieces, parts))
    chip_sum = jnp.sum(exchanged(pieces, "x").astype(F32), 0)
    top, bottom = chip_sum[:, : CHIP // 2], chip_sum[:, CHIP // 2 :]
    keep, give = jnp.where(first, top, bottom), jnp.where(first, bottom, top)
    got = shift(give, "c", 1)
    new = jnp.where(first, jnp.concatenate([keep, got], 2), jnp.concatenate([got, keep], 2))

    branch = jnp.sum(parts.astype(F32), 0).astype(BF16).T.reshape(*inputs.shape[:2], D // Y)
    return (branch, ascent_in, ascent_out, new[0], new[1])


def solution(mesh):
    grid = Mesh(mesh.devices.reshape(Z, X, C, Y), ("z", "x", "c", "y"))
    dp = ("z", "x", "c")

    return jax.shard_map(
        local,
        mesh=grid,
        in_specs=(P(None, dp, None), P(None, dp, None)) + (P(dp, "y"),) * 4,
        out_specs=(P(None, dp, "y"),) + (P(dp, "y"),) * 4,
        check_vma=False,
    )
```

```python
import functools
import math

import jax
import jax.numpy as jnp
from jax import lax
from jax.experimental import pallas as pl
from jax.experimental.pallas import tpu as pltpu
from jax.sharding import Mesh, PartitionSpec as P


D = 1280
FF = 5120

RHO = 0.1
ETA = 0.01


Z, X, C, Y = 8, 4, 2, 4
CHIP = D // (Z * X)
COL = CHIP * X
HALF = FF // Y // C
TILE = 256
SIZES = {"z": Z, "x": X, "c": C, "y": Y}
F32, BF16 = jnp.float32, jnp.bfloat16


def shift(a, axis, by):
    n = SIZES[axis]
    return lax.ppermute(a, axis, [(i, (i + by) % n) for i in range(n)])


def exchanged(parts, axis):
    return lax.all_to_all(parts, axis, 0, 0, tiled=True)


def sum_over(part, axes, count):
    return jnp.sum(exchanged(jnp.broadcast_to(part.reshape(1, 1), (count, 1, 1)), axes))


def gelu_parts(pre):
    cdf = 0.5 * (1.0 + lax.erf(pre * 0.7071067811865476))
    dens = jnp.exp(-0.5 * pre * pre) * 0.3989422804014327
    return (pre * cdf, cdf + pre * dens)


def dot(a, b, da, db):
    return lax.dot_general(a, b, (((da,), (db,)), ((), ())), preferred_element_type=F32)


def by_owner(own_ref, came_ref, work):
    steps = pl.num_programs(0) // 2

    @pl.when(pl.program_id(0) < steps)
    def _():
        work(own_ref[...])

    @pl.when(pl.program_id(0) >= steps)
    def _():
        work(came_ref[...])


def act_kernel(own_ref, came_ref, w_ref, act_ref, slope_ref, pre_ref):
    def product(x):
        pre_ref[...] = dot(x, w_ref[...], 1, 0)

    by_owner(own_ref, came_ref, product)

    def some(i, carry):
        rows = pl.ds(pl.multiple_of(i * 16, 16), 16)
        act, slope = gelu_parts(pre_ref[rows])
        act_ref[rows] = act.astype(BF16)
        slope_ref[rows] = slope
        return carry

    lax.fori_loop(0, TILE // 16, some, 0)


def delta_kernel(own_ref, came_ref, w_ref, slope_ref, delta_ref):
    def product(dy):
        delta_ref[...] = (dot(dy, w_ref[...], 1, 0) * slope_ref[...]).astype(BF16)

    by_owner(own_ref, came_ref, product)


def grad_kernel(own_ref, came_ref, d_ref, g_ref):
    half = own_ref.shape[0]
    g_ref[...] = dot(own_ref[...], d_ref[:half], 0, 0) + dot(came_ref[...], d_ref[half:], 0, 0)


def out_kernel(w_ref, act_ref, own_ref, other_ref):
    half = own_ref.shape[1]
    own_ref[...] = dot(w_ref[...], act_ref[:half], 1, 1).astype(BF16)
    other_ref[...] = dot(w_ref[...], act_ref[half:], 1, 1).astype(BF16)


def add_kernel(plan, whole_ref, *refs):
    came, outs = list(refs[: -len(plan)]), refs[-len(plan) :]
    terms = []
    for k, count in plan:
        terms.append((lax.rem(lax.axis_index("z") + k, Z), [came.pop(0) for _ in range(count)]))

    def some(i, carry):
        rows = pl.ds(pl.multiple_of(i * 32, 32), 32)
        for (at, parts), out in zip(terms, outs):
            total = whole_ref[at, rows]
            for part in parts:
                total = total + part[rows].astype(F32)
            out[rows] = total.astype(BF16)
        return carry

    lax.fori_loop(0, COL // 32, some, 0)


def mix_kernel(own_ref, came_ref, out_ref):
    def some(i, carry):
        rows = pl.ds(pl.multiple_of(i * 64, 64), 64)
        out_ref[rows] = (own_ref[rows].astype(F32) + came_ref[rows].astype(F32)).astype(BF16)
        return carry

    lax.fori_loop(0, D // 64, some, 0)


def small(kernel, outs, *operands):
    return pl.pallas_call(
        kernel,
        out_shape=outs,
        in_specs=[pl.BlockSpec(memory_space=pltpu.VMEM)] * len(operands),
        out_specs=[pl.BlockSpec(memory_space=pltpu.VMEM)] * len(outs),
        compiler_params=pltpu.CompilerParams(vmem_limit_bytes=6 << 20),
        cost_estimate=pl.CostEstimate(flops=1 << 19, bytes_accessed=1 << 20, transcendentals=0),
    )(*operands)


def added(whole, plan, *came):
    outs = [jax.ShapeDtypeStruct((COL, HALF), BF16)] * len(plan)
    return small(functools.partial(add_kernel, plan), outs, whole, *came)


def call(kernel, steps, operands, outs, scratch=()):
    def spec(shape, cut, at):
        block = tuple(TILE if i == cut else n for i, n in enumerate(shape))
        return pl.BlockSpec(block, lambda i: tuple(at(i) if j == cut else 0 for j in range(len(shape))))

    shapes = [jax.ShapeDtypeStruct(*o[0]) for o in outs]
    return pl.pallas_call(
        kernel,
        grid=(steps,),
        in_specs=[spec(o.shape, cut, at) for o, cut, at in operands],
        out_specs=[spec(o[0], cut, at) for o, cut, at in outs],
        out_shape=shapes,
        scratch_shapes=list(scratch),
        compiler_params=pltpu.CompilerParams(vmem_limit_bytes=14 << 20),
        cost_estimate=pl.CostEstimate(flops=2 * 1024 * D * HALF, bytes_accessed=8 << 20, transcendentals=0),
    )(*[o[0] for o in operands])


def same(i):
    return i


def local(inputs, cotangent, w_in, w_out, grad_in, grad_out):
    z, c = lax.axis_index("z"), lax.axis_index("c")
    first = c == 0

    scaled_in = (jnp.abs(w_in.astype(F32)) + ETA) * grad_in
    scaled_out = (jnp.abs(w_out.astype(F32)) + ETA) * grad_out
    part = jnp.sum(scaled_in * scaled_in) + jnp.sum(scaled_out * scaled_out)
    part, w_in, w_out, grad_in, grad_out = lax.optimization_barrier((part, w_in, w_out, grad_in, grad_out))
    part = sum_over(part, ("x", "c", "y"), X * C * Y)

    raw = jnp.stack([w_in, grad_in.astype(BF16), w_out, grad_out.astype(BF16)])
    low, high = raw[:, :, :HALF], raw[:, :, HALF:]
    mine, other = jnp.where(first, low, high), jnp.where(first, high, low)
    came = shift(other, "c", 1)
    chip = jnp.where(first, jnp.concatenate([mine, came], 1), jnp.concatenate([came, mine], 1))
    chip, grad_in, grad_out = lax.optimization_barrier((chip, grad_in, grad_out))
    near = [chip] + [shift(chip, "x", -j if j < 3 else 1) for j in range(1, X)]
    x, dy = inputs.reshape(-1, D), cotangent.reshape(-1, D)
    x_came, dy_came = shift(x, "c", 1), shift(dy, "c", 1)
    tokens = x.shape[0]
    count = C * tokens

    total = lax.psum(part, "z")
    factor = math.sqrt(2.0 * D * FF) / jnp.sqrt(total + 1.0)
    ascent_in = factor * ((jnp.abs(w_in.astype(F32)) + ETA) * grad_in)
    ascent_out = factor * ((jnp.abs(w_out.astype(F32)) + ETA) * grad_out)

    def moved(w, g):
        w, g = w.astype(F32), g.astype(F32)
        scale = jnp.abs(w) + ETA
        return (w + RHO * scale * (factor * (scale * g))).astype(BF16)

    def row(which):
        at = lax.axis_index("x")
        by_x = [lax.select_n(at, *[near[(a - b) % X] for b in range(X)]) for a in range(X)]
        return jnp.concatenate([moved(r[which], r[which + 1]) for r in by_x], 0)

    start_in, start_out = row(0), row(2)

    def place(k):
        return lax.rem(z + k, Z)

    def gathered(block, up):
        full = jnp.zeros((Z, COL, HALF), BF16)
        put = lambda full, block, k: lax.dynamic_update_index_in_dim(full, block, place(k), 0)
        full = put(full, block, 0)
        a = b = block
        for k in range(1, Z // 2 + 1):
            if k < Z // 2 or up:
                a = shift(a, "z", -1)
                full = put(full, a, k)
            if k < Z // 2 or not up:
                b = shift(b, "z", 1)
                full = put(full, b, Z - k)
        return full.reshape(D, HALF)

    full_in = gathered(start_in, True)
    full_out = gathered(start_out, False)

    hidden, square = (count, HALF), (D, HALF)
    half = tokens // TILE
    pair = lambda own, came: ((own, 0, lambda i: jnp.minimum(i, half - 1)), (came, 0, lambda i: jnp.maximum(i - half, 0)))
    act, slope = call(
        act_kernel, count // TILE, (*pair(x, x_came), (full_in, None, same)),
        (((hidden, BF16), 0, same), ((hidden, F32), 0, same)), [pltpu.VMEM((TILE, HALF), F32)],
    )
    (whole_out,) = call(
        grad_kernel, D // TILE, ((dy, 1, same), (dy_came, 1, same), (act, None, same)), (((square, F32), 0, same),)
    )
    (delta,) = call(
        delta_kernel, count // TILE, (*pair(dy, dy_came), (full_out, None, same), (slope, 0, same)),
        (((hidden, BF16), 0, same),),
    )
    (whole_in,) = call(
        grad_kernel, D // TILE, ((x, 1, same), (x_came, 1, same), (delta, None, same)), (((square, F32), 0, same),)
    )

    def reduced(whole, up):
        whole = whole.reshape(Z, COL, HALF)
        far = (4, 5) if up else (3, 4)
        a, b = added(whole, ((far[0], 0), (far[1], 0)))
        for step in range(1, Z // 2 - 1):
            k, m = far[0] - step, far[1] + step
            a, b = shift(a, "z", 1), shift(b, "z", -1)
            a, b = added(whole, ((k, 1), (m, 1)), a, b)
        a, b = shift(a, "z", 1), shift(b, "z", -1)
        if up:
            (a,) = added(whole, ((1, 1),), a)
            a = shift(a, "z", 1)
        else:
            (b,) = added(whole, ((Z - 1, 1),), b)
            b = shift(b, "z", -1)
        return added(whole, ((0, 2),), a, b)[0]

    sums = jnp.stack([reduced(whole_in, True), reduced(whole_out, False)])

    out = (((D, tokens), BF16), 0, same)
    own, other = call(out_kernel, D // TILE, ((full_out, 0, same), (act, None, same)), (out, out))
    other = shift(other, "c", 1)
    (mixed,) = small(mix_kernel, [jax.ShapeDtypeStruct((D, tokens), BF16)], own, other)
    parts = exchanged(mixed.reshape(Y, D // Y, tokens), "y")

    pieces = sums.reshape(2, X, CHIP, HALF).swapaxes(0, 1)
    pieces, parts = lax.optimization_barrier((pieces, parts))
    chip_sum = jnp.sum(exchanged(pieces, "x").astype(F32), 0)
    top, bottom = chip_sum[:, : CHIP // 2], chip_sum[:, CHIP // 2 :]
    keep, give = jnp.where(first, top, bottom), jnp.where(first, bottom, top)
    branch = jnp.sum(parts.astype(F32), 0).astype(BF16).T.reshape(*inputs.shape[:2], D // Y)
    give, branch, ascent_in, ascent_out = lax.optimization_barrier((give, branch, ascent_in, ascent_out))
    got = shift(give, "c", 1)
    new = jnp.where(first, jnp.concatenate([keep, got], 2), jnp.concatenate([got, keep], 2))

    return (branch, ascent_in, ascent_out, new[0], new[1])


def solution(mesh):
    grid = Mesh(mesh.devices.reshape(Z, X, C, Y), ("z", "x", "c", "y"))
    dp = ("z", "x", "c")

    return jax.shard_map(
        local,
        mesh=grid,
        in_specs=(P(None, dp, None), P(None, dp, None)) + (P(dp, "y"),) * 4,
        out_specs=(P(None, dp, "y"),) + (P(dp, "y"),) * 4,
        check_vma=False,
    )
```

```python
import functools
import math

import jax
import jax.numpy as jnp
from jax import lax
from jax.experimental import pallas as pl
from jax.experimental.pallas import tpu as pltpu
from jax.sharding import Mesh, PartitionSpec as P


D = 1280
FF = 5120

RHO = 0.1
ETA = 0.01


Z, X, C, Y = 8, 4, 2, 4
CHIP = D // (Z * X)
COL = CHIP * X
HALF = FF // Y // C
TILE = 256
SIZES = {"z": Z, "x": X, "c": C, "y": Y}
F32, BF16 = jnp.float32, jnp.bfloat16


def shift(a, axis, by):
    n = SIZES[axis]
    return lax.ppermute(a, axis, [(i, (i + by) % n) for i in range(n)])


def exchanged(parts, axis):
    return lax.all_to_all(parts, axis, 0, 0, tiled=True)


def sum_over(part, axes, count):
    return jnp.sum(exchanged(jnp.broadcast_to(part.reshape(1, 1), (count, 1, 1)), axes))


def gelu_parts(pre):
    cdf = 0.5 * (1.0 + lax.erf(pre * 0.7071067811865476))
    dens = jnp.exp(-0.5 * pre * pre) * 0.3989422804014327
    return (pre * cdf, cdf + pre * dens)


def dot(a, b, da, db):
    return lax.dot_general(a, b, (((da,), (db,)), ((), ())), preferred_element_type=F32)


def by_owner(own_ref, came_ref, work):
    own = pl.program_id(0) < pl.num_programs(0) // 2
    work(jnp.where(own, own_ref[...], came_ref[...]))


def act_kernel(own_ref, came_ref, w_ref, act_ref, slope_ref):
    def product(x):
        act, slope = gelu_parts(dot(x, w_ref[...], 1, 0))
        act_ref[...] = act.astype(BF16)
        slope_ref[...] = slope

    by_owner(own_ref, came_ref, product)


def delta_kernel(own_ref, came_ref, w_ref, slope_ref, delta_ref):
    def product(dy):
        delta_ref[...] = (dot(dy, w_ref[...], 1, 0) * slope_ref[...]).astype(BF16)

    by_owner(own_ref, came_ref, product)


def grad_kernel(own_ref, came_ref, d_ref, g_ref):
    half = own_ref.shape[0]
    g_ref[...] = dot(own_ref[...], d_ref[:half], 0, 0) + dot(came_ref[...], d_ref[half:], 0, 0)


def out_kernel(w_ref, act_ref, own_ref, other_ref):
    half = own_ref.shape[1]
    own_ref[...] = dot(w_ref[...], act_ref[:half], 1, 1).astype(BF16)
    other_ref[...] = dot(w_ref[...], act_ref[half:], 1, 1).astype(BF16)


def add_kernel(plan, whole_ref, *refs):
    came, outs = list(refs[: -len(plan)]), refs[-len(plan) :]
    terms = []
    for k, count in plan:
        terms.append((lax.rem(lax.axis_index("z") + k, Z), [came.pop(0) for _ in range(count)]))

    def some(i, carry):
        rows = pl.ds(pl.multiple_of(i * 32, 32), 32)
        for (at, parts), out in zip(terms, outs):
            total = whole_ref[at, rows]
            for part in parts:
                total = total + part[rows].astype(F32)
            out[rows] = total.astype(BF16)
        return carry

    lax.fori_loop(0, COL // 32, some, 0)


def mix_kernel(own_ref, came_ref, out_ref):
    def some(i, carry):
        rows = pl.ds(pl.multiple_of(i * 64, 64), 64)
        out_ref[rows] = (own_ref[rows].astype(F32) + came_ref[rows].astype(F32)).astype(BF16)
        return carry

    lax.fori_loop(0, D // 64, some, 0)


def small(kernel, outs, *operands):
    return pl.pallas_call(
        kernel,
        out_shape=outs,
        in_specs=[pl.BlockSpec(memory_space=pltpu.VMEM)] * len(operands),
        out_specs=[pl.BlockSpec(memory_space=pltpu.VMEM)] * len(outs),
        compiler_params=pltpu.CompilerParams(vmem_limit_bytes=6 << 20),
        cost_estimate=pl.CostEstimate(flops=1 << 19, bytes_accessed=1 << 20, transcendentals=0),
    )(*operands)


def added(whole, plan, *came):
    outs = [jax.ShapeDtypeStruct((COL, HALF), BF16)] * len(plan)
    return small(functools.partial(add_kernel, plan), outs, whole, *came)


def call(kernel, steps, operands, outs):
    def spec(shape, cut, at):
        block = tuple(TILE if i == cut else n for i, n in enumerate(shape))
        return pl.BlockSpec(block, lambda i: tuple(at(i) if j == cut else 0 for j in range(len(shape))))

    shapes = [jax.ShapeDtypeStruct(*o[0]) for o in outs]
    return pl.pallas_call(
        kernel,
        grid=(steps,),
        in_specs=[spec(o.shape, cut, at) for o, cut, at in operands],
        out_specs=[spec(o[0], cut, at) for o, cut, at in outs],
        out_shape=shapes,
        compiler_params=pltpu.CompilerParams(vmem_limit_bytes=14 << 20),
        cost_estimate=pl.CostEstimate(flops=2 * 1024 * D * HALF, bytes_accessed=8 << 20, transcendentals=0),
    )(*[o[0] for o in operands])


def same(i):
    return i


def local(inputs, cotangent, w_in, w_out, grad_in, grad_out):
    z, c = lax.axis_index("z"), lax.axis_index("c")
    first = c == 0

    scaled_in = (jnp.abs(w_in.astype(F32)) + ETA) * grad_in
    scaled_out = (jnp.abs(w_out.astype(F32)) + ETA) * grad_out
    part = jnp.sum(scaled_in * scaled_in) + jnp.sum(scaled_out * scaled_out)
    part, w_in, w_out, grad_in, grad_out = lax.optimization_barrier((part, w_in, w_out, grad_in, grad_out))
    part = sum_over(part, ("x", "c", "y"), X * C * Y)

    raw = jnp.stack([w_in, grad_in.astype(BF16), w_out, grad_out.astype(BF16)])
    low, high = raw[:, :, :HALF], raw[:, :, HALF:]
    mine, other = jnp.where(first, low, high), jnp.where(first, high, low)
    came = shift(other, "c", 1)
    chip = jnp.where(first, jnp.concatenate([mine, came], 1), jnp.concatenate([came, mine], 1))
    chip, grad_in, grad_out = lax.optimization_barrier((chip, grad_in, grad_out))
    near = [chip] + [shift(chip, "x", -j if j < 3 else 1) for j in range(1, X)]
    x, dy = inputs.reshape(-1, D), cotangent.reshape(-1, D)
    x_came, dy_came = shift(x, "c", 1), shift(dy, "c", 1)
    tokens = x.shape[0]
    count = C * tokens

    total = sum_over(part, "z", Z)
    factor = math.sqrt(2.0 * D * FF) / jnp.sqrt(total + 1.0)
    ascent_in = factor * ((jnp.abs(w_in.astype(F32)) + ETA) * grad_in)
    ascent_out = factor * ((jnp.abs(w_out.astype(F32)) + ETA) * grad_out)

    def moved(w, g):
        w, g = w.astype(F32), g.astype(F32)
        scale = jnp.abs(w) + ETA
        return (w + RHO * scale * (factor * (scale * g))).astype(BF16)

    def row(which):
        at = lax.axis_index("x")
        by_x = [lax.select_n(at, *[near[(a - b) % X] for b in range(X)]) for a in range(X)]
        return jnp.concatenate([moved(r[which], r[which + 1]) for r in by_x], 0)

    start_in, start_out = row(0), row(2)

    def place(k):
        return lax.rem(z + k, Z)

    def gathered(block, up):
        full = jnp.zeros((Z, COL, HALF), BF16)
        put = lambda full, block, k: lax.dynamic_update_index_in_dim(full, block, place(k), 0)
        full = put(full, block, 0)
        a = b = block
        for k in range(1, Z // 2 + 1):
            if k < Z // 2 or up:
                a = shift(a, "z", -1)
                full = put(full, a, k)
            if k < Z // 2 or not up:
                b = shift(b, "z", 1)
                full = put(full, b, Z - k)
        return full.reshape(D, HALF)

    full_in = gathered(start_in, True)
    full_out = gathered(start_out, False)

    hidden, square = (count, HALF), (D, HALF)
    half = tokens // TILE
    pair = lambda own, came: ((own, 0, lambda i: jnp.minimum(i, half - 1)), (came, 0, lambda i: jnp.maximum(i - half, 0)))
    act, slope = call(
        act_kernel, count // TILE, (*pair(x, x_came), (full_in, None, same)),
        (((hidden, BF16), 0, same), ((hidden, F32), 0, same)),
    )
    (whole_out,) = call(
        grad_kernel, D // TILE, ((dy, 1, same), (dy_came, 1, same), (act, None, same)), (((square, F32), 0, same),)
    )
    (delta,) = call(
        delta_kernel, count // TILE, (*pair(dy, dy_came), (full_out, None, same), (slope, 0, same)),
        (((hidden, BF16), 0, same),),
    )
    (whole_in,) = call(
        grad_kernel, D // TILE, ((x, 1, same), (x_came, 1, same), (delta, None, same)), (((square, F32), 0, same),)
    )

    def reduced(whole, up):
        whole = whole.reshape(Z, COL, HALF)
        far = (4, 5) if up else (3, 4)
        a, b = added(whole, ((far[0], 0), (far[1], 0)))
        for step in range(1, Z // 2 - 1):
            k, m = far[0] - step, far[1] + step
            a, b = shift(a, "z", 1), shift(b, "z", -1)
            a, b = added(whole, ((k, 1), (m, 1)), a, b)
        a, b = shift(a, "z", 1), shift(b, "z", -1)
        if up:
            (a,) = added(whole, ((1, 1),), a)
            a = shift(a, "z", 1)
        else:
            (b,) = added(whole, ((Z - 1, 1),), b)
            b = shift(b, "z", -1)
        return added(whole, ((0, 2),), a, b)[0]

    sums = jnp.stack([reduced(whole_in, True), reduced(whole_out, False)])

    out = (((D, tokens), BF16), 0, same)
    own, other = call(out_kernel, D // TILE, ((full_out, 0, same), (act, None, same)), (out, out))
    other = shift(other, "c", 1)
    (mixed,) = small(mix_kernel, [jax.ShapeDtypeStruct((D, tokens), BF16)], own, other)
    parts = exchanged(mixed.reshape(Y, D // Y, tokens), "y")

    sums = sums.reshape(2, X, CHIP, HALF)

    def piece(j):
        at = lax.rem(lax.axis_index("x") + j, X)
        return lax.dynamic_index_in_dim(sums, at, 1, keepdims=False)

    chip_sum = piece(0).astype(F32)
    for j in range(1, X):
        chip_sum = chip_sum + shift(piece(j), "x", j if j < 3 else -1).astype(F32)
    top, bottom = chip_sum[:, : CHIP // 2], chip_sum[:, CHIP // 2 :]
    keep, give = jnp.where(first, top, bottom), jnp.where(first, bottom, top)
    branch = jnp.sum(parts.astype(F32), 0).astype(BF16).T.reshape(*inputs.shape[:2], D // Y)
    got = shift(give, "c", 1)
    new = jnp.where(first, jnp.concatenate([keep, got], 2), jnp.concatenate([got, keep], 2))

    return (branch, ascent_in, ascent_out, new[0], new[1])


def solution(mesh):
    grid = Mesh(mesh.devices.reshape(Z, X, C, Y), ("z", "x", "c", "y"))
    dp = ("z", "x", "c")

    return jax.shard_map(
        local,
        mesh=grid,
        in_specs=(P(None, dp, None), P(None, dp, None)) + (P(dp, "y"),) * 4,
        out_specs=(P(None, dp, "y"),) + (P(dp, "y"),) * 4,
        check_vma=False,
    )
```

```python
import functools
import math

import jax
import jax.numpy as jnp
from jax import lax
from jax.experimental import pallas as pl
from jax.experimental.pallas import tpu as pltpu
from jax.sharding import Mesh, PartitionSpec as P


D = 1280
FF = 5120

RHO = 0.1
ETA = 0.01


Z, X, C, Y = 8, 4, 2, 4
CHIP = D // (Z * X)
COL = CHIP * X
HALF = FF // Y // C
TILE = 256
SIZES = {"z": Z, "x": X, "c": C, "y": Y}
F32, BF16 = jnp.float32, jnp.bfloat16


def shift(a, axis, by):
    n = SIZES[axis]
    return lax.ppermute(a, axis, [(i, (i + by) % n) for i in range(n)])


def exchanged(parts, axis):
    return lax.all_to_all(parts, axis, 0, 0, tiled=True)


def gelu_parts(pre):
    cdf = 0.5 * (1.0 + lax.erf(pre * 0.7071067811865476))
    dens = jnp.exp(-0.5 * pre * pre) * 0.3989422804014327
    return (pre * cdf, cdf + pre * dens)


def dot(a, b, da, db):
    return lax.dot_general(a, b, (((da,), (db,)), ((), ())), preferred_element_type=F32)


def by_owner(own_ref, came_ref, work):
    own = pl.program_id(0) < pl.num_programs(0) // 2
    work(jnp.where(own, own_ref[...], came_ref[...]))


def act_kernel(own_ref, came_ref, w_ref, act_ref, slope_ref):
    def product(x):
        act, slope = gelu_parts(dot(x, w_ref[...], 1, 0))
        act_ref[...] = act.astype(BF16)
        slope_ref[...] = slope

    by_owner(own_ref, came_ref, product)


def delta_kernel(own_ref, came_ref, w_ref, slope_ref, delta_ref):
    def product(dy):
        delta_ref[...] = (dot(dy, w_ref[...], 1, 0) * slope_ref[...]).astype(BF16)

    by_owner(own_ref, came_ref, product)


def grad_kernel(own_ref, came_ref, d_ref, g_ref):
    half = own_ref.shape[0]
    g_ref[...] = dot(own_ref[...], d_ref[:half], 0, 0) + dot(came_ref[...], d_ref[half:], 0, 0)


def out_kernel(w_ref, act_ref, own_ref, other_ref):
    half = own_ref.shape[1]
    own_ref[...] = dot(w_ref[...], act_ref[:half], 1, 1).astype(BF16)
    other_ref[...] = dot(w_ref[...], act_ref[half:], 1, 1).astype(BF16)


def part_kernel(w_in_ref, g_in_ref, w_out_ref, g_out_ref, out_ref):
    total = jnp.zeros((), F32)
    for w_ref, g_ref in ((w_in_ref, g_in_ref), (w_out_ref, g_out_ref)):
        scaled = (jnp.abs(w_ref[...].astype(F32)) + ETA) * g_ref[...]
        total = total + jnp.sum(scaled * scaled)
    out_ref[...] = jnp.full(out_ref.shape, total, F32)


def part_sum(count, *operands):
    return pl.pallas_call(
        part_kernel,
        name="part",
        out_shape=jax.ShapeDtypeStruct((count, 8, 128), F32),
        grid=(1,),
        in_specs=[pl.BlockSpec(a.shape, lambda i: (0, 0)) for a in operands],
        out_specs=pl.BlockSpec((count, 8, 128), lambda i: (0, 0, 0)),
    )(*operands)


def sum_kernel(parts_ref, out_ref):
    out_ref[...] = jnp.broadcast_to(jnp.sum(parts_ref[...], 0, keepdims=True), out_ref.shape)


def factor_kernel(parts_ref, out_ref):
    out_ref[...] = math.sqrt(2.0 * D * FF) / jnp.sqrt(jnp.sum(parts_ref[...], 0) + 1.0)


def add_kernel(plan, whole_ref, *refs):
    came, outs = list(refs[: -len(plan)]), refs[-len(plan) :]
    terms = []
    for k, count, _ in plan:
        terms.append((lax.rem(lax.axis_index("z") + k, Z), [came.pop(0) for _ in range(count)]))

    def some(i, carry):
        rows = pl.ds(pl.multiple_of(i * 32, 32), 32)
        for (at, parts), out in zip(terms, outs):
            total = whole_ref[at, rows]
            for part in parts:
                total = total + part[rows].astype(F32)
            out[rows] = total.astype(out.dtype)
        return carry

    lax.fori_loop(0, COL // 32, some, 0)


def mix_kernel(*refs):
    def some(i, carry):
        rows = pl.ds(pl.multiple_of(i * 32, 32), 32)
        total = refs[0][rows].astype(F32)
        for part in refs[1:-1]:
            total = total + part[rows].astype(F32)
        refs[-1][rows] = total.astype(BF16)
        return carry

    lax.fori_loop(0, refs[0].shape[0] // 32, some, 0)


def small(kernel, outs, *operands):
    return pl.pallas_call(
        kernel,
        out_shape=outs,
        in_specs=[pl.BlockSpec(memory_space=pltpu.VMEM)] * len(operands),
        out_specs=[pl.BlockSpec(memory_space=pltpu.VMEM)] * len(outs),
        compiler_params=pltpu.CompilerParams(vmem_limit_bytes=6 << 20),
        cost_estimate=pl.CostEstimate(flops=1 << 19, bytes_accessed=1 << 20, transcendentals=0),
    )(*operands)


def added(whole, plan, *came):
    outs = [jax.ShapeDtypeStruct((COL, HALF), kind) for _, _, kind in plan]
    return small(functools.partial(add_kernel, plan), outs, whole, *came)


def call(kernel, steps, operands, outs):
    def spec(shape, cut, at):
        block = tuple(TILE if i == cut else n for i, n in enumerate(shape))
        return pl.BlockSpec(block, lambda i: tuple(at(i) if j == cut else 0 for j in range(len(shape))))

    shapes = [jax.ShapeDtypeStruct(*o[0]) for o in outs]
    return pl.pallas_call(
        kernel,
        grid=(steps,),
        in_specs=[spec(o.shape, cut, at) for o, cut, at in operands],
        out_specs=[spec(o[0], cut, at) for o, cut, at in outs],
        out_shape=shapes,
        compiler_params=pltpu.CompilerParams(vmem_limit_bytes=14 << 20),
        cost_estimate=pl.CostEstimate(flops=2 * 1024 * D * HALF, bytes_accessed=8 << 20, transcendentals=0),
    )(*[o[0] for o in operands])


def same(i):
    return i


def local(inputs, cotangent, w_in, w_out, grad_in, grad_out):
    z, c = lax.axis_index("z"), lax.axis_index("c")
    first = c == 0

    parts = part_sum(X * C * Y, w_in, grad_in, w_out, grad_out)
    parts, w_in, w_out, grad_in, grad_out = lax.optimization_barrier((parts, w_in, w_out, grad_in, grad_out))
    parts = exchanged(parts, ("x", "c", "y"))
    (parts,) = small(sum_kernel, [jax.ShapeDtypeStruct((Z, 8, 128), F32)], parts)

    raw = jnp.stack([w_in, grad_in.astype(BF16), w_out, grad_out.astype(BF16)])
    low, high = raw[:, :, :HALF], raw[:, :, HALF:]
    mine, other = jnp.where(first, low, high), jnp.where(first, high, low)
    came = shift(other, "c", 1)
    chip = jnp.where(first, jnp.concatenate([mine, came], 1), jnp.concatenate([came, mine], 1))
    chip, grad_in, grad_out = lax.optimization_barrier((chip, grad_in, grad_out))
    near = [chip] + [shift(chip, "x", -j if j < 3 else 1) for j in range(1, X)]
    x, dy = inputs.reshape(-1, D), cotangent.reshape(-1, D)
    x_came, dy_came = shift(x, "c", 1), shift(dy, "c", 1)
    tokens = x.shape[0]
    count = C * tokens

    (factor,) = small(factor_kernel, [jax.ShapeDtypeStruct((8, 128), F32)], exchanged(parts, "z"))
    factor = factor[0, 0]
    ascent_in = factor * ((jnp.abs(w_in.astype(F32)) + ETA) * grad_in)
    ascent_out = factor * ((jnp.abs(w_out.astype(F32)) + ETA) * grad_out)

    def moved(w, g):
        w, g = w.astype(F32), g.astype(F32)
        scale = jnp.abs(w) + ETA
        return (w + RHO * scale * (factor * (scale * g))).astype(BF16)

    def row(which):
        at = lax.axis_index("x")
        by_x = [lax.select_n(at, *[near[(a - b) % X] for b in range(X)]) for a in range(X)]
        return jnp.concatenate([moved(r[which], r[which + 1]) for r in by_x], 0)

    start_in, start_out = row(0), row(2)

    def place(k):
        return lax.rem(z + k, Z)

    def gathered(block, up):
        full = jnp.zeros((Z, COL, HALF), BF16)
        put = lambda full, block, k: lax.dynamic_update_index_in_dim(full, block, place(k), 0)
        full = put(full, block, 0)
        a = b = block
        for k in range(1, Z // 2 + 1):
            if k < Z // 2 or up:
                a = shift(a, "z", -1)
                full = put(full, a, k)
            if k < Z // 2 or not up:
                b = shift(b, "z", 1)
                full = put(full, b, Z - k)
        return full.reshape(D, HALF)

    full_in = gathered(start_in, True)
    full_out = gathered(start_out, False)

    hidden, square = (count, HALF), (D, HALF)
    half = tokens // TILE
    pair = lambda own, came: ((own, 0, lambda i: jnp.minimum(i, half - 1)), (came, 0, lambda i: jnp.maximum(i - half, 0)))
    act, slope = call(
        act_kernel, count // TILE, (*pair(x, x_came), (full_in, None, same)),
        (((hidden, BF16), 0, same), ((hidden, F32), 0, same)),
    )
    (whole_out,) = call(
        grad_kernel, D // TILE, ((dy, 1, same), (dy_came, 1, same), (act, None, same)), (((square, F32), 0, same),)
    )
    (delta,) = call(
        delta_kernel, count // TILE, (*pair(dy, dy_came), (full_out, None, same), (slope, 0, same)),
        (((hidden, BF16), 0, same),),
    )
    (whole_in,) = call(
        grad_kernel, D // TILE, ((x, 1, same), (x_came, 1, same), (delta, None, same)), (((square, F32), 0, same),)
    )

    def reduced(whole, up):
        whole = whole.reshape(Z, COL, HALF)
        far = (4, 5) if up else (3, 4)
        a, b, own = added(whole, ((far[0], 0, BF16), (far[1], 0, BF16), (0, 0, F32)))
        for step in range(1, Z // 2 - 1):
            k, m = far[0] - step, far[1] + step
            a, b = shift(a, "z", 1), shift(b, "z", -1)
            a, b = added(whole, ((k, 1, BF16), (m, 1, BF16)), a, b)
        a, b = shift(a, "z", 1), shift(b, "z", -1)
        if up:
            (a,) = added(whole, ((1, 1, BF16),), a)
            a = shift(a, "z", 1)
        else:
            (b,) = added(whole, ((Z - 1, 1, BF16),), b)
            b = shift(b, "z", -1)
        return small(mix_kernel, [jax.ShapeDtypeStruct((COL, HALF), BF16)], own, a, b)[0]

    sums = jnp.stack([reduced(whole_in, True), reduced(whole_out, False)])

    out = (((D, tokens), BF16), 0, same)
    own, other = call(out_kernel, D // TILE, ((full_out, 0, same), (act, None, same)), (out, out))
    other = shift(other, "c", 1)
    (mixed,) = small(mix_kernel, [jax.ShapeDtypeStruct((D, tokens), BF16)], own, other)
    parts = exchanged(mixed.reshape(Y, D // Y, tokens), "y")

    sums = sums.reshape(2, X, CHIP, HALF)

    def piece(j):
        at = lax.rem(lax.axis_index("x") + j, X)
        return lax.dynamic_index_in_dim(sums, at, 1, keepdims=False)

    chip_sum = piece(0).astype(F32)
    for j in range(1, X):
        chip_sum = chip_sum + shift(piece(j), "x", j if j < 3 else -1).astype(F32)
    top, bottom = chip_sum[:, : CHIP // 2], chip_sum[:, CHIP // 2 :]
    keep, give = jnp.where(first, top, bottom), jnp.where(first, bottom, top)
    branch = jnp.sum(parts.astype(F32), 0).astype(BF16)
    branch = branch.T.reshape(*inputs.shape[:2], D // Y)
    got = shift(give, "c", 1)
    new = jnp.where(first, jnp.concatenate([keep, got], 2), jnp.concatenate([got, keep], 2))

    return (branch, ascent_in, ascent_out, new[0], new[1])


def solution(mesh):
    grid = Mesh(mesh.devices.reshape(Z, X, C, Y), ("z", "x", "c", "y"))
    dp = ("z", "x", "c")

    return jax.shard_map(
        local,
        mesh=grid,
        in_specs=(P(None, dp, None), P(None, dp, None)) + (P(dp, "y"),) * 4,
        out_specs=(P(None, dp, "y"),) + (P(dp, "y"),) * 4,
        check_vma=False,
    )
```

```python
import functools
import math

import jax
import jax.numpy as jnp
from jax import lax
from jax.experimental import pallas as pl
from jax.experimental.pallas import tpu as pltpu
from jax.sharding import Mesh, PartitionSpec as P


D = 1280
FF = 5120

RHO = 0.1
ETA = 0.01


Z, X, C, Y = 8, 4, 2, 4
CHIP = D // (Z * X)
COL = CHIP * X
HALF = FF // Y // C
TILE = 256
SIZES = {"z": Z, "x": X, "c": C, "y": Y}
F32, BF16 = jnp.float32, jnp.bfloat16


def shift(a, axis, by):
    n = SIZES[axis]
    return lax.ppermute(a, axis, [(i, (i + by) % n) for i in range(n)])


def exchanged(parts, axis):
    return lax.all_to_all(parts, axis, 0, 0, tiled=True)


def gelu_parts(pre):
    cdf = 0.5 * (1.0 + lax.erf(pre * 0.7071067811865476))
    dens = jnp.exp(-0.5 * pre * pre) * 0.3989422804014327
    return (pre * cdf, cdf + pre * dens)


def dot(a, b, da, db):
    return lax.dot_general(a, b, (((da,), (db,)), ((), ())), preferred_element_type=F32)


def by_owner(own_ref, came_ref, work):
    own = pl.program_id(0) < pl.num_programs(0) // 2
    work(jnp.where(own, own_ref[...], came_ref[...]))


def act_kernel(own_ref, came_ref, w_ref, act_ref, slope_ref):
    def product(x):
        act, slope = gelu_parts(dot(x, w_ref[...], 1, 0))
        act_ref[...] = act.astype(BF16)
        slope_ref[...] = slope

    by_owner(own_ref, came_ref, product)


def delta_kernel(own_ref, came_ref, w_ref, slope_ref, delta_ref):
    def product(dy):
        delta_ref[...] = (dot(dy, w_ref[...], 1, 0) * slope_ref[...]).astype(BF16)

    by_owner(own_ref, came_ref, product)


def grad_kernel(own_ref, came_ref, d_ref, g_ref):
    half = own_ref.shape[0]
    g_ref[...] = dot(own_ref[...], d_ref[:half], 0, 0) + dot(came_ref[...], d_ref[half:], 0, 0)


def out_kernel(w_ref, act_ref, own_ref, other_ref):
    half = own_ref.shape[1]
    own_ref[...] = dot(w_ref[...], act_ref[:half], 1, 1).astype(BF16)
    other_ref[...] = dot(w_ref[...], act_ref[half:], 1, 1).astype(BF16)


def part_kernel(w_in_ref, g_in_ref, w_out_ref, g_out_ref, sum_ref, mine_ref, other_ref):
    total = jnp.zeros((), F32)
    for w_ref, g_ref in ((w_in_ref, g_in_ref), (w_out_ref, g_out_ref)):
        scaled = (jnp.abs(w_ref[...].astype(F32)) + ETA) * g_ref[...]
        total = total + jnp.sum(scaled * scaled)
    sum_ref[...] = jnp.full(sum_ref.shape, total, F32)
    c = lax.axis_index("c")
    for i, ref in enumerate((w_in_ref, g_in_ref, w_out_ref, g_out_ref)):
        mine_ref[i] = ref[:, pl.ds(pl.multiple_of(c * HALF, 128), HALF)].astype(BF16)
        other_ref[i] = ref[:, pl.ds(pl.multiple_of((1 - c) * HALF, 128), HALF)].astype(BF16)


def part_sum(count, *operands):
    half = (len(operands), operands[0].shape[0], HALF)
    outs = (((count, 8, 128), F32), (half, BF16), (half, BF16))
    return pl.pallas_call(
        part_kernel,
        name="part",
        out_shape=[jax.ShapeDtypeStruct(*o) for o in outs],
        grid=(1,),
        in_specs=[pl.BlockSpec(a.shape, lambda i: (0, 0)) for a in operands],
        out_specs=[pl.BlockSpec(shape, lambda i: (0, 0, 0)) for shape, _ in outs],
    )(*operands)


def moved_kernel(*refs):
    near, factor = refs[:X], refs[X][0, 0]
    x = lax.axis_index("x")
    for which, out in ((0, refs[X + 1]), (2, refs[X + 2])):
        for j, ref in enumerate(near):
            w, g = ref[which].astype(F32), ref[which + 1].astype(F32)
            scale = jnp.abs(w) + ETA
            out[lax.rem(x + j, X)] = (w + RHO * scale * (factor * (scale * g))).astype(BF16)


def sum_kernel(parts_ref, out_ref):
    out_ref[...] = jnp.broadcast_to(jnp.sum(parts_ref[...], 0, keepdims=True), out_ref.shape)


def factor_kernel(parts_ref, out_ref):
    out_ref[...] = math.sqrt(2.0 * D * FF) / jnp.sqrt(jnp.sum(parts_ref[...], 0) + 1.0)


def add_kernel(plan, whole_ref, *refs):
    came, outs = list(refs[: -len(plan)]), refs[-len(plan) :]
    terms = []
    for k, count, _ in plan:
        terms.append((lax.rem(lax.axis_index("z") + k, Z), [came.pop(0) for _ in range(count)]))

    def some(i, carry):
        rows = pl.ds(pl.multiple_of(i * 32, 32), 32)
        for (at, parts), out in zip(terms, outs):
            total = whole_ref[at, rows]
            for part in parts:
                total = total + part[rows].astype(F32)
            out[rows] = total.astype(out.dtype)
        return carry

    lax.fori_loop(0, COL // 32, some, 0)


def mix_kernel(*refs):
    def some(i, carry):
        rows = pl.ds(pl.multiple_of(i * 32, 32), 32)
        total = refs[0][rows].astype(F32)
        for part in refs[1:-1]:
            total = total + part[rows].astype(F32)
        refs[-1][rows] = total.astype(BF16)
        return carry

    lax.fori_loop(0, refs[0].shape[0] // 32, some, 0)


def small(kernel, outs, *operands):
    return pl.pallas_call(
        kernel,
        out_shape=outs,
        in_specs=[pl.BlockSpec(memory_space=pltpu.VMEM)] * len(operands),
        out_specs=[pl.BlockSpec(memory_space=pltpu.VMEM)] * len(outs),
        compiler_params=pltpu.CompilerParams(vmem_limit_bytes=6 << 20),
        cost_estimate=pl.CostEstimate(flops=1 << 19, bytes_accessed=1 << 20, transcendentals=0),
    )(*operands)


def added(whole, plan, *came):
    outs = [jax.ShapeDtypeStruct((COL, HALF), kind) for _, _, kind in plan]
    return small(functools.partial(add_kernel, plan), outs, whole, *came)


def call(kernel, steps, operands, outs):
    def spec(shape, cut, at):
        block = tuple(TILE if i == cut else n for i, n in enumerate(shape))
        return pl.BlockSpec(block, lambda i: tuple(at(i) if j == cut else 0 for j in range(len(shape))))

    shapes = [jax.ShapeDtypeStruct(*o[0]) for o in outs]
    return pl.pallas_call(
        kernel,
        grid=(steps,),
        in_specs=[spec(o.shape, cut, at) for o, cut, at in operands],
        out_specs=[spec(o[0], cut, at) for o, cut, at in outs],
        out_shape=shapes,
        compiler_params=pltpu.CompilerParams(vmem_limit_bytes=14 << 20),
        cost_estimate=pl.CostEstimate(flops=2 * 1024 * D * HALF, bytes_accessed=8 << 20, transcendentals=0),
    )(*[o[0] for o in operands])


def same(i):
    return i


def local(inputs, cotangent, w_in, w_out, grad_in, grad_out):
    z, c = lax.axis_index("z"), lax.axis_index("c")
    first = c == 0

    parts, mine, other = part_sum(X * C * Y, w_in, grad_in, w_out, grad_out)
    parts = exchanged(parts, ("x", "c", "y"))
    (parts,) = small(sum_kernel, [jax.ShapeDtypeStruct((Z, 8, 128), F32)], parts)

    came = shift(other, "c", 1)
    chip = jnp.where(first, jnp.concatenate([mine, came], 1), jnp.concatenate([came, mine], 1))
    chip, grad_in, grad_out = lax.optimization_barrier((chip, grad_in, grad_out))
    near = [chip] + [shift(chip, "x", -j if j < 3 else 1) for j in range(1, X)]
    x, dy = inputs.reshape(-1, D), cotangent.reshape(-1, D)
    x_came, dy_came = shift(x, "c", 1), shift(dy, "c", 1)
    tokens = x.shape[0]
    count = C * tokens

    (factor,) = small(factor_kernel, [jax.ShapeDtypeStruct((8, 128), F32)], exchanged(parts, "z"))
    rows = small(moved_kernel, [jax.ShapeDtypeStruct((X, CHIP, HALF), BF16)] * 2, *near, factor)
    start_in, start_out = (r.reshape(COL, HALF) for r in rows)
    factor = factor[0, 0]
    ascent_in = factor * ((jnp.abs(w_in.astype(F32)) + ETA) * grad_in)
    ascent_out = factor * ((jnp.abs(w_out.astype(F32)) + ETA) * grad_out)

    def place(k):
        return lax.rem(z + k, Z)

    def gathered(block, up):
        full = jnp.zeros((Z, COL, HALF), BF16)
        put = lambda full, block, k: lax.dynamic_update_index_in_dim(full, block, place(k), 0)
        full = put(full, block, 0)
        a = b = block
        for k in range(1, Z // 2 + 1):
            if k < Z // 2 or up:
                a = shift(a, "z", -1)
                full = put(full, a, k)
            if k < Z // 2 or not up:
                b = shift(b, "z", 1)
                full = put(full, b, Z - k)
        return full.reshape(D, HALF)

    full_in = gathered(start_in, True)
    full_out = gathered(start_out, False)

    hidden, square = (count, HALF), (D, HALF)
    half = tokens // TILE
    pair = lambda own, came: ((own, 0, lambda i: jnp.minimum(i, half - 1)), (came, 0, lambda i: jnp.maximum(i - half, 0)))
    act, slope = call(
        act_kernel, count // TILE, (*pair(x, x_came), (full_in, None, same)),
        (((hidden, BF16), 0, same), ((hidden, F32), 0, same)),
    )
    (whole_out,) = call(
        grad_kernel, D // TILE, ((dy, 1, same), (dy_came, 1, same), (act, None, same)), (((square, F32), 0, same),)
    )
    (delta,) = call(
        delta_kernel, count // TILE, (*pair(dy, dy_came), (full_out, None, same), (slope, 0, same)),
        (((hidden, BF16), 0, same),),
    )
    (whole_in,) = call(
        grad_kernel, D // TILE, ((x, 1, same), (x_came, 1, same), (delta, None, same)), (((square, F32), 0, same),)
    )

    def reduced(whole, up):
        whole = whole.reshape(Z, COL, HALF)
        far = (4, 5) if up else (3, 4)
        a, b, own = added(whole, ((far[0], 0, BF16), (far[1], 0, BF16), (0, 0, F32)))
        for step in range(1, Z // 2 - 1):
            k, m = far[0] - step, far[1] + step
            a, b = shift(a, "z", 1), shift(b, "z", -1)
            a, b = added(whole, ((k, 1, BF16), (m, 1, BF16)), a, b)
        a, b = shift(a, "z", 1), shift(b, "z", -1)
        if up:
            (a,) = added(whole, ((1, 1, BF16),), a)
            a = shift(a, "z", 1)
        else:
            (b,) = added(whole, ((Z - 1, 1, BF16),), b)
            b = shift(b, "z", -1)
        return small(mix_kernel, [jax.ShapeDtypeStruct((COL, HALF), BF16)], own, a, b)[0]

    sums = jnp.stack([reduced(whole_in, True), reduced(whole_out, False)])

    out = (((D, tokens), BF16), 0, same)
    own, other = call(out_kernel, D // TILE, ((full_out, 0, same), (act, None, same)), (out, out))
    other = shift(other, "c", 1)
    (mixed,) = small(mix_kernel, [jax.ShapeDtypeStruct((D, tokens), BF16)], own, other)
    parts = exchanged(mixed.reshape(Y, D // Y, tokens), "y")

    sums = sums.reshape(2, X, CHIP, HALF)

    def piece(j):
        at = lax.rem(lax.axis_index("x") + j, X)
        return lax.dynamic_index_in_dim(sums, at, 1, keepdims=False)

    chip_sum = piece(0).astype(F32)
    for j in range(1, X):
        chip_sum = chip_sum + shift(piece(j), "x", j if j < 3 else -1).astype(F32)
    top, bottom = chip_sum[:, : CHIP // 2], chip_sum[:, CHIP // 2 :]
    keep, give = jnp.where(first, top, bottom), jnp.where(first, bottom, top)
    branch = jnp.sum(parts.astype(F32), 0).astype(BF16)
    branch = branch.T.reshape(*inputs.shape[:2], D // Y)
    got = shift(give, "c", 1)
    new = jnp.where(first, jnp.concatenate([keep, got], 2), jnp.concatenate([got, keep], 2))

    return (branch, ascent_in, ascent_out, new[0], new[1])


def solution(mesh):
    grid = Mesh(mesh.devices.reshape(Z, X, C, Y), ("z", "x", "c", "y"))
    dp = ("z", "x", "c")

    return jax.shard_map(
        local,
        mesh=grid,
        in_specs=(P(None, dp, None), P(None, dp, None)) + (P(dp, "y"),) * 4,
        out_specs=(P(None, dp, "y"),) + (P(dp, "y"),) * 4,
        check_vma=False,
    )
```

```python
import functools
import math

import jax
import jax.numpy as jnp
from jax import lax
from jax.experimental import pallas as pl
from jax.experimental.pallas import tpu as pltpu
from jax.sharding import Mesh, PartitionSpec as P


D = 1280
FF = 5120

RHO = 0.1
ETA = 0.01


Z, X, C, Y = 8, 4, 2, 4
CHIP = D // (Z * X)
COL = CHIP * X
HALF = FF // Y // C
TILE = 256
SIZES = {"z": Z, "x": X, "c": C, "y": Y}
F32, BF16 = jnp.float32, jnp.bfloat16


def shift(a, axis, by):
    n = SIZES[axis]
    return lax.ppermute(a, axis, [(i, (i + by) % n) for i in range(n)])


def exchanged(parts, axis):
    return lax.all_to_all(parts, axis, 0, 0, tiled=True)


def gelu_parts(pre):
    cdf = 0.5 * (1.0 + lax.erf(pre * 0.7071067811865476))
    dens = jnp.exp(-0.5 * pre * pre) * 0.3989422804014327
    return (pre * cdf, cdf + pre * dens)


def dot(a, b, da, db):
    return lax.dot_general(a, b, (((da,), (db,)), ((), ())), preferred_element_type=F32)


def by_owner(own_ref, came_ref, work):
    own = pl.program_id(0) < pl.num_programs(0) // 2
    work(jnp.where(own, own_ref[...], came_ref[...]))


def act_kernel(own_ref, came_ref, w_ref, act_ref, slope_ref):
    def product(x):
        act, slope = gelu_parts(dot(x, w_ref[...], 1, 0))
        act_ref[...] = act.astype(BF16)
        slope_ref[...] = slope

    by_owner(own_ref, came_ref, product)


def delta_kernel(own_ref, came_ref, w_ref, slope_ref, delta_ref):
    def product(dy):
        delta_ref[...] = (dot(dy, w_ref[...], 1, 0) * slope_ref[...]).astype(BF16)

    by_owner(own_ref, came_ref, product)


def grad_kernel(own_ref, came_ref, d_ref, g_ref):
    half = own_ref.shape[0]
    g_ref[...] = dot(own_ref[...], d_ref[:half], 0, 0) + dot(came_ref[...], d_ref[half:], 0, 0)


def out_kernel(w_ref, act_ref, own_ref, other_ref):
    half = own_ref.shape[1]
    own_ref[...] = dot(w_ref[...], act_ref[:half], 1, 1).astype(BF16)
    other_ref[...] = dot(w_ref[...], act_ref[half:], 1, 1).astype(BF16)


def part_kernel(w_in_ref, g_in_ref, w_out_ref, g_out_ref, sum_ref, mine_ref, other_ref):
    total = jnp.zeros((), F32)
    for w_ref, g_ref in ((w_in_ref, g_in_ref), (w_out_ref, g_out_ref)):
        scaled = (jnp.abs(w_ref[...].astype(F32)) + ETA) * g_ref[...]
        total = total + jnp.sum(scaled * scaled)
    sum_ref[...] = jnp.full(sum_ref.shape, total, F32)
    c = lax.axis_index("c")
    for i, ref in enumerate((w_in_ref, g_in_ref, w_out_ref, g_out_ref)):
        mine_ref[i] = ref[:, pl.ds(pl.multiple_of(c * HALF, 128), HALF)].astype(BF16)
        other_ref[i] = ref[:, pl.ds(pl.multiple_of((1 - c) * HALF, 128), HALF)].astype(BF16)


def part_sum(count, *operands):
    half = (len(operands), operands[0].shape[0], HALF)
    outs = (((count, 8, 128), F32), (half, BF16), (half, BF16))
    return pl.pallas_call(
        part_kernel,
        name="part",
        out_shape=[jax.ShapeDtypeStruct(*o) for o in outs],
        grid=(1,),
        in_specs=[pl.BlockSpec(a.shape, lambda i: (0, 0)) for a in operands],
        out_specs=[pl.BlockSpec(shape, lambda i: (0, 0, 0)) for shape, _ in outs],
    )(*operands)


def ascent_kernel(factor_ref, w_in_ref, g_in_ref, w_out_ref, g_out_ref, in_ref, out_ref):
    factor = factor_ref[0, 0]
    in_ref[...] = factor * ((jnp.abs(w_in_ref[...].astype(F32)) + ETA) * g_in_ref[...])
    out_ref[...] = factor * ((jnp.abs(w_out_ref[...].astype(F32)) + ETA) * g_out_ref[...])


def ascents(*operands):
    spec = lambda a: pl.BlockSpec(a.shape, lambda i: (0, 0))
    return pl.pallas_call(
        ascent_kernel,
        name="ascent",
        out_shape=[jax.ShapeDtypeStruct(operands[2].shape, F32)] * 2,
        grid=(1,),
        in_specs=[spec(a) for a in operands],
        out_specs=[spec(operands[2])] * 2,
        compiler_params=pltpu.CompilerParams(vmem_limit_bytes=6 << 20),
        cost_estimate=pl.CostEstimate(flops=1 << 19, bytes_accessed=1 << 20, transcendentals=0),
    )(*operands)


def moved_kernel(*refs):
    near, factor = refs[:X], refs[X][0, 0]
    x = lax.axis_index("x")
    for which, out in ((0, refs[X + 1]), (2, refs[X + 2])):
        for j, ref in enumerate(near):
            w, g = ref[which].astype(F32), ref[which + 1].astype(F32)
            scale = jnp.abs(w) + ETA
            out[lax.rem(x + j, X)] = (w + RHO * scale * (factor * (scale * g))).astype(BF16)


def sum_kernel(parts_ref, out_ref):
    out_ref[...] = jnp.broadcast_to(jnp.sum(parts_ref[...], 0, keepdims=True), out_ref.shape)


def factor_kernel(parts_ref, out_ref):
    out_ref[...] = math.sqrt(2.0 * D * FF) / jnp.sqrt(jnp.sum(parts_ref[...], 0) + 1.0)


def add_kernel(plan, whole_ref, *refs):
    came, outs = list(refs[: -len(plan)]), refs[-len(plan) :]
    terms = []
    for k, count, _ in plan:
        terms.append((lax.rem(lax.axis_index("z") + k, Z), [came.pop(0) for _ in range(count)]))

    def some(i, carry):
        rows = pl.ds(pl.multiple_of(i * 32, 32), 32)
        for (at, parts), out in zip(terms, outs):
            total = whole_ref[at, rows]
            for part in parts:
                total = total + part[rows].astype(F32)
            out[rows] = total.astype(out.dtype)
        return carry

    lax.fori_loop(0, COL // 32, some, 0)


def mix_kernel(*refs):
    def some(i, carry):
        rows = pl.ds(pl.multiple_of(i * 32, 32), 32)
        total = refs[0][rows].astype(F32)
        for part in refs[1:-1]:
            total = total + part[rows].astype(F32)
        refs[-1][rows] = total.astype(BF16)
        return carry

    lax.fori_loop(0, refs[0].shape[0] // 32, some, 0)


def small(kernel, outs, *operands):
    return pl.pallas_call(
        kernel,
        out_shape=outs,
        in_specs=[pl.BlockSpec(memory_space=pltpu.VMEM)] * len(operands),
        out_specs=[pl.BlockSpec(memory_space=pltpu.VMEM)] * len(outs),
        compiler_params=pltpu.CompilerParams(vmem_limit_bytes=6 << 20),
        cost_estimate=pl.CostEstimate(flops=1 << 19, bytes_accessed=1 << 20, transcendentals=0),
    )(*operands)


def added(whole, plan, *came):
    outs = [jax.ShapeDtypeStruct((COL, HALF), kind) for _, _, kind in plan]
    return small(functools.partial(add_kernel, plan), outs, whole, *came)


def call(kernel, steps, operands, outs):
    def spec(shape, cut, at):
        block = tuple(TILE if i == cut else n for i, n in enumerate(shape))
        return pl.BlockSpec(block, lambda i: tuple(at(i) if j == cut else 0 for j in range(len(shape))))

    shapes = [jax.ShapeDtypeStruct(*o[0]) for o in outs]
    return pl.pallas_call(
        kernel,
        grid=(steps,),
        in_specs=[spec(o.shape, cut, at) for o, cut, at in operands],
        out_specs=[spec(o[0], cut, at) for o, cut, at in outs],
        out_shape=shapes,
        compiler_params=pltpu.CompilerParams(vmem_limit_bytes=14 << 20),
        cost_estimate=pl.CostEstimate(flops=2 * 1024 * D * HALF, bytes_accessed=8 << 20, transcendentals=0),
    )(*[o[0] for o in operands])


def same(i):
    return i


def local(inputs, cotangent, w_in, w_out, grad_in, grad_out):
    z, c = lax.axis_index("z"), lax.axis_index("c")
    first = c == 0

    parts, mine, other = part_sum(X * C * Y, w_in, grad_in, w_out, grad_out)
    parts = exchanged(parts, ("x", "c", "y"))
    (parts,) = small(sum_kernel, [jax.ShapeDtypeStruct((Z, 8, 128), F32)], parts)

    came = shift(other, "c", 1)
    chip = jnp.where(first, jnp.concatenate([mine, came], 1), jnp.concatenate([came, mine], 1))
    near = [chip] + [shift(chip, "x", -j if j < 3 else 1) for j in range(1, X)]
    x, dy = inputs.reshape(-1, D), cotangent.reshape(-1, D)
    x_came, dy_came = shift(x, "c", 1), shift(dy, "c", 1)
    tokens = x.shape[0]
    count = C * tokens

    (factor,) = small(factor_kernel, [jax.ShapeDtypeStruct((8, 128), F32)], exchanged(parts, "z"))
    rows = small(moved_kernel, [jax.ShapeDtypeStruct((X, CHIP, HALF), BF16)] * 2, *near, factor)
    start_in, start_out = (r.reshape(COL, HALF) for r in rows)
    ascent_in, ascent_out = ascents(factor, w_in, grad_in, w_out, grad_out)

    def place(k):
        return lax.rem(z + k, Z)

    def gathered(block, up):
        full = jnp.zeros((Z, COL, HALF), BF16)
        put = lambda full, block, k: lax.dynamic_update_index_in_dim(full, block, place(k), 0)
        full = put(full, block, 0)
        a = b = block
        for k in range(1, Z // 2 + 1):
            if k < Z // 2 or up:
                a = shift(a, "z", -1)
                full = put(full, a, k)
            if k < Z // 2 or not up:
                b = shift(b, "z", 1)
                full = put(full, b, Z - k)
        return full.reshape(D, HALF)

    full_in = gathered(start_in, True)
    full_out = gathered(start_out, False)

    hidden, square = (count, HALF), (D, HALF)
    half = tokens // TILE
    pair = lambda own, came: ((own, 0, lambda i: jnp.minimum(i, half - 1)), (came, 0, lambda i: jnp.maximum(i - half, 0)))
    act, slope = call(
        act_kernel, count // TILE, (*pair(x, x_came), (full_in, None, same)),
        (((hidden, BF16), 0, same), ((hidden, F32), 0, same)),
    )
    (whole_out,) = call(
        grad_kernel, D // TILE, ((dy, 1, same), (dy_came, 1, same), (act, None, same)), (((square, F32), 0, same),)
    )
    (delta,) = call(
        delta_kernel, count // TILE, (*pair(dy, dy_came), (full_out, None, same), (slope, 0, same)),
        (((hidden, BF16), 0, same),),
    )
    (whole_in,) = call(
        grad_kernel, D // TILE, ((x, 1, same), (x_came, 1, same), (delta, None, same)), (((square, F32), 0, same),)
    )

    def reduced(whole, up):
        whole = whole.reshape(Z, COL, HALF)
        far = (4, 5) if up else (3, 4)
        a, b, own = added(whole, ((far[0], 0, BF16), (far[1], 0, BF16), (0, 0, F32)))
        for step in range(1, Z // 2 - 1):
            k, m = far[0] - step, far[1] + step
            a, b = shift(a, "z", 1), shift(b, "z", -1)
            a, b = added(whole, ((k, 1, BF16), (m, 1, BF16)), a, b)
        a, b = shift(a, "z", 1), shift(b, "z", -1)
        if up:
            (a,) = added(whole, ((1, 1, BF16),), a)
            a = shift(a, "z", 1)
        else:
            (b,) = added(whole, ((Z - 1, 1, BF16),), b)
            b = shift(b, "z", -1)
        return small(mix_kernel, [jax.ShapeDtypeStruct((COL, HALF), BF16)], own, a, b)[0]

    sums = jnp.stack([reduced(whole_in, True), reduced(whole_out, False)])

    out = (((D, tokens), BF16), 0, same)
    own, other = call(out_kernel, D // TILE, ((full_out, 0, same), (act, None, same)), (out, out))
    other = shift(other, "c", 1)
    (mixed,) = small(mix_kernel, [jax.ShapeDtypeStruct((D, tokens), BF16)], own, other)
    parts = exchanged(mixed.reshape(Y, D // Y, tokens), "y")

    sums = sums.reshape(2, X, CHIP, HALF)

    def piece(j):
        at = lax.rem(lax.axis_index("x") + j, X)
        return lax.dynamic_index_in_dim(sums, at, 1, keepdims=False)

    chip_sum = piece(0).astype(F32)
    for j in range(1, X):
        chip_sum = chip_sum + shift(piece(j), "x", j if j < 3 else -1).astype(F32)
    top, bottom = chip_sum[:, : CHIP // 2], chip_sum[:, CHIP // 2 :]
    keep, give = jnp.where(first, top, bottom), jnp.where(first, bottom, top)
    branch = jnp.sum(parts.astype(F32), 0).astype(BF16)
    branch = branch.T.reshape(*inputs.shape[:2], D // Y)
    got = shift(give, "c", 1)
    new = jnp.where(first, jnp.concatenate([keep, got], 2), jnp.concatenate([got, keep], 2))

    return (branch, ascent_in, ascent_out, new[0], new[1])


def solution(mesh):
    grid = Mesh(mesh.devices.reshape(Z, X, C, Y), ("z", "x", "c", "y"))
    dp = ("z", "x", "c")

    return jax.shard_map(
        local,
        mesh=grid,
        in_specs=(P(None, dp, None), P(None, dp, None)) + (P(dp, "y"),) * 4,
        out_specs=(P(None, dp, "y"),) + (P(dp, "y"),) * 4,
        check_vma=False,
    )
```
